32 devices in a mesh: gx: 2 (over x), gy: 4 (over y, core), gz: 4 (over z).
Axes of the slice: x: 2, y: 2, z: 4, core: 2. Of those that a mesh axis runs over, the one named last changes fastest.
Arguments:
- vorticity: float32 [3, 16, 64, 512], P(None, 'gx', 'gy', 'gz'), may hold values from -6 to 6
- velocity: float32 [3, 16, 64, 512], P(None, 'gx', 'gy', 'gz'), may hold values from -1 to 1
Outputs:
- vorticity_out: float32 [3, 16, 64, 512], P(None, 'gx', 'gy', 'gz')
The draws below stay inside these ranges and needn't reach their ends.
All inputs are finite; a program needn't handle non-finite values.
Results may differ from the reference program's by a relative error of at most 0.0003.
Values sent between devices are 32-bit elements; how exact they have to be, the bound alone decides.
A program may use at most 64 MiB of HBM per device.

```python
import jax
import jax.numpy as jnp

SUBSTEPS = 2
NX = 16
NY = 64
NZ = 512


def level_of(key, shape, shards, least, largest):
    def one(position, blocks):
        heights = jax.random.uniform(jax.random.fold_in(jax.random.fold_in(key, 6), position), (blocks,), jnp.float32, least / len(shards), largest / len(shards))
        return jnp.repeat(jnp.exp(heights), shape[position] // blocks).reshape((-1,) + (1,) * (len(shape) - position - 1))

    gain = one(*shards[0])
    for cut in shards[1:]:
        gain = gain * one(*cut)
    return gain


def bell_draw(stream_key, extent, deviation, bound, split=(), held_as=jnp.bfloat16):
    factor_of = level_of(stream_key, extent, split, -0.22, 0.18) if split else 1.0
    array = jax.random.normal(stream_key, extent, jnp.float32) * deviation * factor_of
    return jnp.minimum(jnp.maximum(array, -bound), bound).astype(held_as)


def setup_inputs(seed: int = 0) -> dict:
    splits = jax.random.split(jax.random.key(seed), 3)
    vorticity = bell_draw(splits[0], (3, NX, NY, NZ), 1.0, 6.0, ((1, 2), (2, 4), (3, 4)), jnp.float32)
    velocity = jnp.clip(jax.random.uniform(splits[1], (3, NX, NY, NZ), jnp.float32, -1.0, 1.0) * level_of(splits[1], (3, NX, NY, NZ), ((1, 2), (2, 4), (3, 4)), -0.4, 0.0), -1.0, 1.0)
    return dict(vorticity=vorticity, velocity=velocity)


time_step = 0.5


def kernel(distance):
    magnitude = jnp.abs(distance)
    near = 1.0 - 2.5 * magnitude * magnitude + 1.5 * magnitude * magnitude * magnitude
    far = 0.5 * (2.0 - magnitude) * (2.0 - magnitude) * (1.0 - magnitude)
    return jnp.where(magnitude < 1.0, near, jnp.where(magnitude < 2.0, far, 0.0))


def remesh(current, displace, along):
    total = jnp.zeros_like(current)
    for offset in range(-2, 3):
        total = total + jnp.roll(kernel(offset - displace) * current, offset, axis=along)
    return total


def derive(values, along):
    near_diff = jnp.roll(values, -1, axis=along) - jnp.roll(values, 1, axis=along)
    far_diff = jnp.roll(values, -2, axis=along) - jnp.roll(values, 2, axis=along)
    return (8.0 * near_diff - far_diff) / 12.0


def reference(vorticity, velocity):
    slopes = [derive(velocity, along) for along in (1, 2, 3)]
    current = vorticity
    for substep in range(SUBSTEPS):
        for along in (1, 2, 3):
            current = remesh(current, time_step * velocity[along - 1], along)
        stretch = current[0] * slopes[0] + current[1] * slopes[1] + current[2] * slopes[2]
        current = current + time_step * stretch
    return current
```

```python
import functools

import jax
import jax.numpy as jnp
from jax import lax
from jax.experimental import pallas as pl
from jax.experimental.pallas import tpu as pltpu
from jax.sharding import PartitionSpec as P

SUBSTEPS = 2
TIME_STEP = 0.5
AXES = ("gx", "gy", "gz")
MESH = pl.DeviceIdType.MESH


def roll(values, shift, axis):
    return pltpu.roll(values, shift % values.shape[axis], axis)


def weights(velocity):
    d = TIME_STEP * velocity
    s = jnp.abs(d)
    t = 1.0 - s
    positive = d > 0.0
    centre = 1.0 + s * s * (1.5 * s - 2.5)
    toward = 1.0 + t * t * (1.5 * t - 2.5)
    away = -0.5 * s * t * t
    beyond = -0.5 * s * s * t
    return (
        jnp.where(positive, 0.0, beyond),
        jnp.where(positive, away, toward),
        centre,
        jnp.where(positive, toward, away),
        jnp.where(positive, beyond, 0.0),
    )


def body(
    sizes, vort, vel, out, wgt, slope, cur, sx, rx, sy, ry, sz, rz, rvx, svy, rvy, svz, rvz,
    send_sem, recv_sem,
):
    _, X, Y, Z = vort.shape
    here = [lax.axis_index(a) for a in AXES]

    def neighbour(k, side):
        n = sizes[k]
        moved = lax.rem(here[k] + (1 if side else n - 1), n)
        return tuple(moved if j == k else here[j] for j in range(3))

    def push(src, dst, index, k, side):
        copy = pltpu.make_async_remote_copy(
            src_ref=src, dst_ref=dst, send_sem=send_sem.at[index], recv_sem=recv_sem.at[index],
            device_id=neighbour(k, side), device_id_type=MESH,
        )
        copy.start()
        return copy

    barrier = pltpu.get_barrier_semaphore()
    for k in range(3):
        for side in range(2):
            pl.semaphore_signal(barrier, inc=1, device_id=neighbour(k, side), device_id_type=MESH)

    lane = lax.broadcasted_iota(jnp.int32, (8, Z), 1)
    lane3 = lax.broadcasted_iota(jnp.int32, (X, Y, Z), 2)
    row3 = lax.broadcasted_iota(jnp.int32, (X, Y, Z), 1)
    slabs = [(c, x, y) for c in range(3) for x in range(X) for y in range(0, Y, 8)]
    per = Z // 4

    def pack(edges, target):
        for m in range(0, len(slabs), per):
            held = jnp.zeros((8, Z), jnp.float32)
            for k, (c, x, y) in enumerate(slabs[m:m + per]):
                moved = roll(edges[c][x, y:y + 8, :], 4 * k + 2, 1)
                held = jnp.where(lane // 4 == k, moved, held)
            target[m // per] = held

    def unpack(low_side, high_side):
        merged = [
            jnp.where(lane % 4 >= 2, low_side[m], high_side[m])
            for m in range(-(-len(slabs) // per))
        ]
        edge = (lane < 2) | (lane >= Z - 2)
        return [
            jnp.where(edge, roll(merged[i // per], -(4 * (i % per) + 2), 1), 0.0)
            for i in range(len(slabs))
        ]

    def spread_x(src, step):
        for c in range(3):
            w = [wgt.at[0, a] for a in range(5)]
            sx[step, 0, c, 0] = w[0][0] * src[c, 0]
            sx[step, 0, c, 1] = w[1][0] * src[c, 0] + w[0][1] * src[c, 1]
            sx[step, 1, c, 0] = w[3][X - 1] * src[c, X - 1] + w[4][X - 2] * src[c, X - 2]
            sx[step, 1, c, 1] = w[4][X - 1] * src[c, X - 1]

    def interior_x(src):
        for c in range(3):
            layers = []
            for x in range(X):
                total = None
                for a in range(-2, 3):
                    if 0 <= x - a < X:
                        term = wgt[0, a + 2, x - a] * src[c, x - a]
                        total = term if total is None else total + term
                layers.append(total)
            for x in range(X):
                yield c, x, layers[x]

    def put_weights(k):
        for a, w in enumerate(weights(vel[k])):
            wgt[k, a] = w

    put_weights(0)
    spread_x(vort, 0)
    pl.semaphore_wait(barrier, 6)
    pending = []
    first = [push(sx.at[0, s], rx.at[0, s], s, 0, s) for s in range(2)]
    for s in range(2):
        svy[s] = vel[:, :, pl.ds((Y - 2) * s, 2), :]
    pack([vel[c] for c in range(3)], svz)
    vy = [push(svy.at[s], rvy.at[s], 14 + s, 1, s) for s in range(2)]
    vz = [push(svz, rvz.at[s], 16 + s, 2, s) for s in range(2)]
    vx = [push(vel.at[:, pl.ds((X - 2) * s, 2)], rvx.at[s], 12 + s, 0, s) for s in range(2)]
    put_weights(1)
    put_weights(2)

    scale = TIME_STEP / 12.0

    def slopes_y():
        for c in range(3):
            v = vel[c]
            near = 8.0 * (roll(v, -1, 1) - roll(v, 1, 1)) - (roll(v, -2, 1) - roll(v, 2, 1))
            slope[1, c] = near * scale
        for cp in vy:
            cp.wait()
        for c in range(3):
            top = vel[c, :, 0:4, :]
            low = rvy[1, c]
            slope[1, c, :, 0:1, :] = scale * (
                8.0 * (top[:, 1:2] - low[:, 1:2]) - (top[:, 2:3] - low[:, 0:1]))
            slope[1, c, :, 1:2, :] = scale * (
                8.0 * (top[:, 2:3] - top[:, 0:1]) - (top[:, 3:4] - low[:, 1:2]))
            end = vel[c, :, Y - 4:Y, :]
            high = rvy[0, c]
            slope[1, c, :, Y - 2:Y - 1, :] = scale * (
                8.0 * (end[:, 3:4] - end[:, 1:2]) - (high[:, 0:1] - end[:, 0:1]))
            slope[1, c, :, Y - 1:Y, :] = scale * (
                8.0 * (high[:, 0:1] - end[:, 2:3]) - (high[:, 1:2] - end[:, 1:2]))

    def slopes_z():
        for cp in vz:
            cp.wait()
        halo = unpack(rvz.at[0], rvz.at[1])
        for i, (c, x, y) in enumerate(slabs):
            v = vel[c, x, y:y + 8, :]
            h = halo[i]

            def at(shift):
                source = roll(v, -shift, 1)
                if shift > 0:
                    return jnp.where(lane >= Z - shift, roll(h, -shift, 1), source)
                return jnp.where(lane < -shift, roll(h, -shift, 1), source)

            slope[2, c, x, y:y + 8, :] = scale * (8.0 * (at(1) - at(-1)) - (at(2) - at(-2)))

    def slopes_x():
        for cp in vx:
            cp.wait()
        for c in range(3):
            def layer(x):
                if x < 0:
                    return rvx[1, c, x + 2]
                if x >= X:
                    return rvx[0, c, x - X]
                return vel[c, x]
            for x in range(X):
                slope[0, c, x] = scale * (
                    8.0 * (layer(x + 1) - layer(x - 1)) - (layer(x + 2) - layer(x - 2)))

    for step in range(SUBSTEPS):
        base = step * 6
        src = vort if step == 0 else cur
        if step > 0:
            spread_x(src, step)
            first = [push(sx.at[step, s], rx.at[step, s], base + s, 0, s) for s in range(2)]
        for c, x, layer in interior_x(src):
            cur[c, x] = layer
        if step == 0:
            slopes_y()
            slopes_z()
        for cp in first:
            cp.wait()
        for c in range(3):
            for x in range(2):
                cur[c, x] += rx[step, 1, c, x]
                cur[c, X - 2 + x] += rx[step, 0, c, x]

        for c in range(3):
            v = cur[c]
            u = [wgt[1, a] * v for a in range(5)]
            keep, go = u[2], None
            for a in (-2, -1, 1, 2):
                moved = roll(u[a + 2], a, 1)
                outside = row3 < a if a > 0 else row3 >= Y + a
                keep = keep + jnp.where(outside, 0.0, moved)
                part = jnp.where(outside, moved, 0.0)
                go = part if go is None else go + part
            cur[c] = keep
            sy[step, 1, c] = go[:, 0:2, :]
            sy[step, 0, c] = go[:, Y - 2:Y, :]
        copies = [push(sy.at[step, s], ry.at[step, s], base + 2 + s, 1, s) for s in range(2)]
        if step == 0:
            slopes_x()
        for cp in copies:
            cp.wait()
        for c in range(3):
            cur[c, :, 0:2, :] += ry[step, 1, c]
            cur[c, :, Y - 2:Y, :] += ry[step, 0, c]

        edges = []
        for c in range(3):
            v = cur[c]
            u = [wgt[2, a] * v for a in range(5)]
            keep, go = u[2], None
            for a in (-2, -1, 1, 2):
                moved = roll(u[a + 2], a, 2)
                outside = lane3 < a if a > 0 else lane3 >= Z + a
                keep = keep + jnp.where(outside, 0.0, moved)
                part = jnp.where(outside, moved, 0.0)
                go = part if go is None else go + part
            cur[c] = keep
            edges.append(go)
        pack(edges, sz.at[step])
        copies = [push(sz.at[step], rz.at[step, s], base + 4 + s, 2, s) for s in range(2)]
        for cp in copies:
            cp.wait()
        halo = unpack(rz.at[step, 1], rz.at[step, 0])
        final = out if step == SUBSTEPS - 1 else cur
        for x in range(X):
            for y in range(0, Y, 8):
                v = [
                    cur[c, x, y:y + 8, :] + halo[slabs.index((c, x, y))]
                    for c in range(3)
                ]
                for i in range(3):
                    total = v[i]
                    for j in range(3):
                        total = total + v[j] * slope[j, i, x, y:y + 8, :]
                    final[i, x, y:y + 8, :] = total


def solution(mesh):
    sizes = [mesh.shape[a] for a in AXES]

    def local(vort, vel):
        _, X, Y, Z = vort.shape
        packs = -(-(3 * X * (Y // 8)) // (Z // 4))
        f32 = jnp.float32
        V = pltpu.VMEM
        S = SUBSTEPS
        return pl.pallas_call(
            functools.partial(body, sizes),
            out_shape=jax.ShapeDtypeStruct(vort.shape, f32),
            in_specs=[pl.BlockSpec(memory_space=pltpu.VMEM)] * 2,
            out_specs=pl.BlockSpec(memory_space=pltpu.VMEM),
            scratch_shapes=[
                V((3, 5, X, Y, Z), f32),
                V((3, 3, X, Y, Z), f32),
                V((3, X, Y, Z), f32),
                V((S, 2, 3, 2, Y, Z), f32),
                V((S, 2, 3, 2, Y, Z), f32),
                V((S, 2, 3, X, 2, Z), f32),
                V((S, 2, 3, X, 2, Z), f32),
                V((S, packs, 8, Z), f32),
                V((S, 2, packs, 8, Z), f32),
                V((2, 3, 2, Y, Z), f32),
                V((2, 3, X, 2, Z), f32),
                V((2, 3, X, 2, Z), f32),
                V((packs, 8, Z), f32),
                V((2, packs, 8, Z), f32),
                pltpu.SemaphoreType.DMA((18,)),
                pltpu.SemaphoreType.DMA((18,)),
            ],
            compiler_params=pltpu.CompilerParams(collective_id=0, has_side_effects=True),
        )(vort, vel)

    placed = P(None, *AXES)
    return jax.shard_map(
        local, mesh=mesh, in_specs=(placed, placed), out_specs=placed, check_vma=False
    )
```

```python
import functools

import jax
import jax.numpy as jnp
from jax import lax
from jax.experimental import pallas as pl
from jax.experimental.pallas import tpu as pltpu
from jax.sharding import PartitionSpec as P

SUBSTEPS = 2
TIME_STEP = 0.5
AXES = ("gx", "gy", "gz")
MESH = pl.DeviceIdType.MESH


def roll(values, shift, axis):
    return pltpu.roll(values, shift % values.shape[axis], axis)


def weights(velocity):
    d = TIME_STEP * velocity
    s = jnp.abs(d)
    t = 1.0 - s
    positive = d > 0.0
    centre = 1.0 + s * s * (1.5 * s - 2.5)
    toward = 1.0 + t * t * (1.5 * t - 2.5)
    away = -0.5 * s * t * t
    beyond = -0.5 * s * s * t
    return (
        jnp.where(positive, 0.0, beyond),
        jnp.where(positive, away, toward),
        centre,
        jnp.where(positive, toward, away),
        jnp.where(positive, beyond, 0.0),
    )


def body(
    sizes, vort, vel, out, wgt, slope, cur, sx, rx, sy, ry, sxy, rxy, szi, rzi, szx, rzx,
    rvx, svy, rvy, svz, rvz, wyh, send_sem, recv_sem,
):
    _, X, Y, Z = vort.shape
    here = [lax.axis_index(a) for a in AXES]
    f32 = jnp.float32
    both = (-1, 1)
    three = (-1, 0, 1)
    xdirs = (1,) if sizes[0] == 2 else both
    used = [0]

    def device(offset):
        return tuple(
            h if o == 0 else lax.rem(h + (o if o > 0 else n + o), n)
            for h, o, n in zip(here, offset, sizes)
        )

    def push(src, dst, offset):
        index = used[0]
        used[0] += 1
        copy = pltpu.make_async_remote_copy(
            src_ref=src, dst_ref=dst, send_sem=send_sem.at[index], recv_sem=recv_sem.at[index],
            device_id=device(offset), device_id_type=MESH,
        )
        copy.start()
        return copy

    def done(copies):
        for copy in copies:
            copy.wait()

    barrier = pltpu.get_barrier_semaphore()
    greeted = 0
    for dz in three:
        for dy in three:
            for dx in (0,) + xdirs:
                if dx or dy or dz:
                    pl.semaphore_signal(
                        barrier, inc=1, device_id=device((dx, dy, dz)), device_id_type=MESH)
                    greeted += 1

    lane = lax.broadcasted_iota(jnp.int32, (Y, Z), 1)
    lane3 = lax.broadcasted_iota(jnp.int32, (X, Y, Z), 2)
    row3 = lax.broadcasted_iota(jnp.int32, (X, Y, Z), 1)
    edge = (lane < 2) | (lane >= Z - 2)

    def pack(entries):
        held = jnp.zeros((Y, Z), f32)
        for k, values in entries:
            held = jnp.where(lane // 4 == k, roll(values, 4 * k + 2, 1), held)
        return held

    def unpack(packed, k):
        return jnp.where(edge, roll(packed, -(4 * k + 2), 1), 0.0)

    def put_weights(k):
        for a, w in zip(range(-2, 3), weights(vel[k])):
            if k and a:
                at, n = (row3, Y) if k == 1 else (lane3, Z)
                w = jnp.where(at >= n - a if a > 0 else at < -a, 0.0, w)
            wgt[k, a + 2] = w

    def side_of(d):
        return (d + 1) // 2

    def tile(dy):
        return pl.ds(0, Y) if dy == 0 else pl.ds(0 if dy < 0 else Y - 8, 8)

    def spread_x(src, step):
        for c in range(3):
            sx[step, 0, c, 0] = wgt[0, 0, 0] * src[c, 0]
            sx[step, 0, c, 1] = wgt[0, 1, 0] * src[c, 0] + wgt[0, 0, 1] * src[c, 1]
            sx[step, 1, c, 0] = wgt[0, 3, X - 1] * src[c, X - 1] + wgt[0, 4, X - 2] * src[c, X - 2]
            sx[step, 1, c, 1] = wgt[0, 4, X - 1] * src[c, X - 1]
        for s in range(2):
            for t in range(2):
                sxy[step, s, t] = sx[step, s, :, :, (Y - 2) * t:(Y - 2) * t + 2, :]
        szx[step] = pack([
            (c * X + (0 if s else X - 2) + x, sx[step, s, c, x])
            for s in range(2) for c in range(3) for x in range(2)
        ])

    def interior_x(src, step):
        for c in range(3):
            layers = []
            for x in range(X):
                total = None
                for a in range(-2, 3):
                    if 0 <= x - a < X:
                        term = wgt[0, a + 2, x - a] * src[c, x - a]
                        total = term if total is None else total + term
                layers.append(total)
            for x in range(X):
                cur[c, x] = layers[x]
        for t in range(2):
            sy[step, t] = cur[:, :, (Y - 2) * t:(Y - 2) * t + 2, :]
        szi[step] = pack([(c * X + x, cur[c, x]) for c in range(3) for x in range(X)])

    def send_x(step):
        diagonal = [
            push(szx.at[step, tile(dy)],
                 rzx.at[step, i, side_of(dz), dy + 1, pl.ds(0, 8 if dy else Y)], (dx, dy, dz))
            for dy in (-1, 1, 0) for dz in both for i, dx in enumerate(xdirs)
        ]
        corner = [
            push(sxy.at[step, side_of(dx), side_of(dy)],
                 rxy.at[step, side_of(dx), side_of(dy)], (dx, dy, 0))
            for dx in both for dy in both
        ]
        face = [
            push(sx.at[step, side_of(dx)], rx.at[step, side_of(dx)], (dx, 0, 0)) for dx in both
        ]
        return diagonal, corner, face

    def send_packs(src, dst):
        return [
            push(src.at[tile(dy)], dst.at[side_of(dz), dy + 1, pl.ds(0, 8 if dy else Y)], (0, dy, dz))
            for dy in (-1, 1, 0) for dz in both
        ]

    def send_rows(src, dst):
        return [push(src.at[side_of(dy)], dst.at[side_of(dy)], (0, dy, 0)) for dy in both]

    put_weights(0)
    spread_x(vort, 0)
    interior_x(vort, 0)
    for t in range(2):
        svy[t] = vel[:, :, (Y - 2) * t:(Y - 2) * t + 2, :]
    svz[...] = pack([(c * X + x, vel[c, x]) for c in range(3) for x in range(X)])
    pl.semaphore_wait(barrier, greeted)

    diagonal, corner, face = send_x(0)
    rows = send_rows(sy.at[0], ry.at[0])
    packs = send_packs(szi.at[0], rzi.at[0])
    vrows = send_rows(svy, rvy)
    vpacks = send_packs(svz, rvz)
    vface = [
        push(vel.at[:, pl.ds((X - 2) * s, 2)], rvx.at[s], (2 * s - 1, 0, 0)) for s in range(2)
    ]
    put_weights(1)
    put_weights(2)

    scale = TIME_STEP / 12.0
    low_lanes = lane % 4 < 2

    def merge(received, dy):
        count = 8 if dy else Y
        return jnp.where(low_lanes[:count], received[1, dy + 1, :count], received[0, dy + 1, :count])

    def stack(received):
        return jnp.concatenate([merge(received, dy) for dy in (1, 0, -1)], axis=0)

    def repeat(packed, k):
        n = 4 * X
        at = lax.broadcasted_iota(jnp.int32, packed.shape, 1)
        full = jnp.zeros(packed.shape, f32)
        for c in range(3):
            full = jnp.where((at >= c * n) & (at < (c + 1) * n), roll(packed, (c - k) * n, 1), full)
        return full

    def slopes_y():
        for c in range(3):
            v = vel[c]
            slope[1, c] = scale * (
                8.0 * (roll(v, -1, 1) - roll(v, 1, 1)) - (roll(v, -2, 1) - roll(v, 2, 1)))
        done(vrows)
        for c in range(3):
            top = vel[c, :, 0:4, :]
            low = rvy[1, c]
            slope[1, c, :, 0:1, :] = scale * (
                8.0 * (top[:, 1:2] - low[:, 1:2]) - (top[:, 2:3] - low[:, 0:1]))
            slope[1, c, :, 1:2, :] = scale * (
                8.0 * (top[:, 2:3] - top[:, 0:1]) - (top[:, 3:4] - low[:, 1:2]))
            end = vel[c, :, Y - 4:Y, :]
            high = rvy[0, c]
            slope[1, c, :, Y - 2:Y - 1, :] = scale * (
                8.0 * (end[:, 3:4] - end[:, 1:2]) - (high[:, 0:1] - end[:, 0:1]))
            slope[1, c, :, Y - 1:Y, :] = scale * (
                8.0 * (high[:, 0:1] - end[:, 2:3]) - (high[:, 1:2] - end[:, 1:2]))
        for s in range(2):
            w = weights(rvy[s, 1])
            wyh[s, 0] = w[3] if s else w[1]
            wyh[s, 1] = w[4] if s else w[0]

    def slopes_z(halo):
        for c in range(3):
            for x in range(X):
                v = vel[c, x]
                h = roll(halo, -(4 * (c * X + x) + 2), 1)

                def at(shift):
                    mask = lane < shift if shift > 0 else lane >= Z + shift
                    return roll(jnp.where(mask, h, v), -shift, 1)

                slope[2, c, x] = scale * (8.0 * (at(1) - at(-1)) - (at(2) - at(-2)))

    def slopes_x():
        done(vface)
        for c in range(3):
            def layer(x):
                if x < 0:
                    return rvx[1, c, x + 2]
                if x >= X:
                    return rvx[0, c, x - X]
                return vel[c, x]
            for x in range(X):
                slope[0, c, x] = scale * (
                    8.0 * (layer(x + 1) - layer(x - 1)) - (layer(x + 2) - layer(x - 2)))

    wy_packed = wz_packed = None
    for step in range(SUBSTEPS):
        if step > 0:
            spread_x(cur, step)
            diagonal, corner, face = send_x(step)
            interior_x(cur, step)
            rows = send_rows(sy.at[step], ry.at[step])
            packs = send_packs(szi.at[step], rzi.at[step])
        if step == 0:
            slopes_y()
        done(rows)
        done(corner)
        for s in range(2):
            ry[step, s, :, 0:2] += rxy[step, 1, s]
            ry[step, s, :, X - 2:X] += rxy[step, 0, s]
        done(face)
        for c in range(3):
            for x in range(2):
                cur[c, x] += rx[step, 1, c, x]
                cur[c, X - 2 + x] += rx[step, 0, c, x]

        for c in range(3):
            v = cur[c]
            keep = wgt[1, 2] * v
            for a in (-2, -1, 1, 2):
                keep = keep + roll(wgt[1, a + 2] * v, a, 1)
            cur[c] = keep
            low, high = ry[step, 1, c], ry[step, 0, c]
            near, far = wyh[1, 0] * low, wyh[1, 1] * low
            cur[c, :, 0:1, :] += near[:, 1:2] + far[:, 0:1]
            cur[c, :, 1:2, :] += far[:, 1:2]
            near, far = wyh[0, 0] * high, wyh[0, 1] * high
            cur[c, :, Y - 1:Y, :] += near[:, 0:1] + far[:, 1:2]
            cur[c, :, Y - 2:Y - 1, :] += far[:, 0:1]
        for c in range(3):
            v = cur[c]
            keep = wgt[2, 2] * v
            for a in (-2, -1, 1, 2):
                keep = keep + roll(wgt[2, a + 2] * v, a, 2)
            cur[c] = keep

        if step == 0:
            done(vpacks)
            vpacked = stack(rvz)
            wy_packed = weights(repeat(vpacked, 1))
            wz_packed = [w[8:8 + Y] for w in weights(repeat(vpacked, 2))]
            slopes_z(vpacked[8:8 + Y])
            slopes_x()

        done(packs)
        done(diagonal)
        halo = stack(rzi.at[step])
        if len(xdirs) == 1:
            halo = halo + stack(rzx.at[step, 0])
        else:
            x_of = (lax.broadcasted_iota(jnp.int32, halo.shape, 1) // 4) % X
            halo = halo + jnp.where(x_of >= X - 2, stack(rzx.at[step, 0]), 0.0)
            halo = halo + jnp.where(x_of < 2, stack(rzx.at[step, 1]), 0.0)
        spread = wy_packed[2] * halo
        for a in (-2, -1, 1, 2):
            spread = spread + roll(wy_packed[a + 2] * halo, a, 0)
        spread = spread[8:8 + Y]
        up = roll(wz_packed[4] * spread, 2, 1) + jnp.where(
            lane % 4 == 2, roll(wz_packed[3] * spread, 1, 1), 0.0)
        down = roll(wz_packed[0] * spread, -2, 1) + jnp.where(
            lane % 4 == 1, roll(wz_packed[1] * spread, -1, 1), 0.0)
        ghosts = jnp.where(low_lanes, down, up)

        final = out if step == SUBSTEPS - 1 else cur
        for x in range(X):
            v = [cur[c, x] + unpack(ghosts, c * X + x) for c in range(3)]
            for i in range(3):
                total = v[i]
                for j in range(3):
                    total = total + v[j] * slope[j, i, x]
                final[i, x] = total


def solution(mesh):
    sizes = [mesh.shape[a] for a in AXES]

    def local(vort, vel):
        _, X, Y, Z = vort.shape
        assert 12 * X <= Z and Y % 8 == 0
        f32 = jnp.float32
        V = pltpu.VMEM
        S = SUBSTEPS
        xdirs = 1 if sizes[0] == 2 else 2
        messages = S * (2 + 2 + 4 + 6 + 6 * xdirs) + 2 + 2 + 6
        return pl.pallas_call(
            functools.partial(body, sizes),
            out_shape=jax.ShapeDtypeStruct(vort.shape, f32),
            in_specs=[pl.BlockSpec(memory_space=pltpu.VMEM)] * 2,
            out_specs=pl.BlockSpec(memory_space=pltpu.VMEM),
            scratch_shapes=[
                V((3, 5, X, Y, Z), f32),
                V((3, 3, X, Y, Z), f32),
                V((3, X, Y, Z), f32),
                V((S, 2, 3, 2, Y, Z), f32),
                V((S, 2, 3, 2, Y, Z), f32),
                V((S, 2, 3, X, 2, Z), f32),
                V((S, 2, 3, X, 2, Z), f32),
                V((S, 2, 2, 3, 2, 2, Z), f32),
                V((S, 2, 2, 3, 2, 2, Z), f32),
                V((S, Y, Z), f32),
                V((S, 2, 3, Y, Z), f32),
                V((S, Y, Z), f32),
                V((S, xdirs, 2, 3, Y, Z), f32),
                V((2, 3, 2, Y, Z), f32),
                V((2, 3, X, 2, Z), f32),
                V((2, 3, X, 2, Z), f32),
                V((Y, Z), f32),
                V((2, 3, Y, Z), f32),
                V((2, 2, X, 2, Z), f32),
                pltpu.SemaphoreType.DMA((messages,)),
                pltpu.SemaphoreType.DMA((messages,)),
            ],
            compiler_params=pltpu.CompilerParams(collective_id=0, has_side_effects=True),
        )(vort, vel)

    placed = P(None, *AXES)
    return jax.shard_map(
        local, mesh=mesh, in_specs=(placed, placed), out_specs=placed, check_vma=False
    )
```

```python
import functools

import jax
import jax.numpy as jnp
from jax import lax
from jax.experimental import pallas as pl
from jax.experimental.pallas import tpu as pltpu
from jax.sharding import PartitionSpec as P

SUBSTEPS = 2
TIME_STEP = 0.5
AXES = ("gx", "gy", "gz")
MESH = pl.DeviceIdType.MESH


def roll(values, shift, axis):
    return pltpu.roll(values, shift % values.shape[axis], axis)


def weights(velocity):
    d = TIME_STEP * velocity
    s = jnp.abs(d)
    t = 1.0 - s
    positive = d > 0.0
    centre = 1.0 + s * s * (1.5 * s - 2.5)
    toward = 1.0 + t * t * (1.5 * t - 2.5)
    away = -0.5 * s * t * t
    beyond = -0.5 * s * s * t
    return (
        jnp.where(positive, 0.0, beyond),
        jnp.where(positive, away, toward),
        centre,
        jnp.where(positive, toward, away),
        jnp.where(positive, beyond, 0.0),
    )


def body(
    sizes, vort_in, vel_in, out, vort, vel, wgt, slope, cur, sx, rx, sy, ry, sxy, rxy, szi, rzi, szx, rzx,
    rvx, svy, rvy, svz, rvz, wyh, send_sem, recv_sem, load_sem,
):
    _, X, Y, Z = vort.shape
    here = [lax.axis_index(a) for a in AXES]
    f32 = jnp.float32
    both = (-1, 1)
    three = (-1, 0, 1)
    xdirs = (1,) if sizes[0] == 2 else both
    used = [0]

    def device(offset):
        return tuple(
            h if o == 0 else lax.rem(h + (o if o > 0 else n + o), n)
            for h, o, n in zip(here, offset, sizes)
        )

    def push(src, dst, offset):
        index = used[0]
        used[0] += 1
        copy = pltpu.make_async_remote_copy(
            src_ref=src, dst_ref=dst, send_sem=send_sem.at[index], recv_sem=recv_sem.at[index],
            device_id=device(offset), device_id_type=MESH,
        )
        copy.start()
        return copy

    def done(copies):
        for copy in copies:
            copy.wait()

    barrier = pltpu.get_barrier_semaphore()
    greeted = 0
    for dz in three:
        for dy in three:
            for dx in (0,) + xdirs:
                if dx or dy or dz:
                    pl.semaphore_signal(
                        barrier, inc=1, device_id=device((dx, dy, dz)), device_id_type=MESH)
                    greeted += 1
    loads = [
        pltpu.make_async_copy(src, dst, load_sem.at[i])
        for i, (src, dst) in enumerate(((vel_in, vel), (vort_in, vort)))
    ]
    for load in loads:
        load.start()

    lane = lax.broadcasted_iota(jnp.int32, (Y, Z), 1)
    lane3 = lax.broadcasted_iota(jnp.int32, (X, Y, Z), 2)
    row3 = lax.broadcasted_iota(jnp.int32, (X, Y, Z), 1)
    edge = (lane < 2) | (lane >= Z - 2)

    def pack(entries):
        held = jnp.zeros((Y, Z), f32)
        for k, values in entries:
            held = jnp.where(lane // 4 == k, roll(values, 4 * k + 2, 1), held)
        return held

    def unpack(packed, k):
        return jnp.where(edge, roll(packed, -(4 * k + 2), 1), 0.0)

    def put_weights(k):
        for a, w in zip(range(-2, 3), weights(vel[k])):
            if k and a:
                at, n = (row3, Y) if k == 1 else (lane3, Z)
                w = jnp.where(at >= n - a if a > 0 else at < -a, 0.0, w)
            wgt[k, a + 2] = w

    def side_of(d):
        return (d + 1) // 2

    def tile(dy):
        return pl.ds(0, Y) if dy == 0 else pl.ds(0 if dy < 0 else Y - 8, 8)

    def spread_x(src, step):
        for c in range(3):
            sx[step, 0, c, 0] = wgt[0, 0, 0] * src[c, 0]
            sx[step, 0, c, 1] = wgt[0, 1, 0] * src[c, 0] + wgt[0, 0, 1] * src[c, 1]
            sx[step, 1, c, 0] = wgt[0, 3, X - 1] * src[c, X - 1] + wgt[0, 4, X - 2] * src[c, X - 2]
            sx[step, 1, c, 1] = wgt[0, 4, X - 1] * src[c, X - 1]
        for s in range(2):
            for t in range(2):
                sxy[step, s, t] = sx[step, s, :, :, (Y - 2) * t:(Y - 2) * t + 2, :]
        szx[step] = pack([
            (c * X + (0 if s else X - 2) + x, sx[step, s, c, x])
            for s in range(2) for c in range(3) for x in range(2)
        ])

    def interior_x(src, step):
        for c in range(3):
            layers = []
            for x in range(X):
                total = None
                for a in range(-2, 3):
                    if 0 <= x - a < X:
                        term = wgt[0, a + 2, x - a] * src[c, x - a]
                        total = term if total is None else total + term
                layers.append(total)
            for x in range(X):
                cur[c, x] = layers[x]
        for t in range(2):
            sy[step, t] = cur[:, :, (Y - 2) * t:(Y - 2) * t + 2, :]
        szi[step] = pack([(c * X + x, cur[c, x]) for c in range(3) for x in range(X)])

    def send_x(step):
        diagonal = [
            push(szx.at[step, tile(dy)],
                 rzx.at[step, i, side_of(dz), dy + 1, pl.ds(0, 8 if dy else Y)], (dx, dy, dz))
            for dy in (-1, 1, 0) for dz in both for i, dx in enumerate(xdirs)
        ]
        corner = [
            push(sxy.at[step, side_of(dx), side_of(dy)],
                 rxy.at[step, side_of(dx), side_of(dy)], (dx, dy, 0))
            for dx in both for dy in both
        ]
        face = [
            push(sx.at[step, side_of(dx)], rx.at[step, side_of(dx)], (dx, 0, 0)) for dx in both
        ]
        return diagonal, corner, face

    def send_packs(src, dst):
        return [
            push(src.at[tile(dy)], dst.at[side_of(dz), dy + 1, pl.ds(0, 8 if dy else Y)], (0, dy, dz))
            for dy in (-1, 1, 0) for dz in both
        ]

    def send_rows(src, dst):
        return [push(src.at[side_of(dy)], dst.at[side_of(dy)], (0, dy, 0)) for dy in both]

    loads[0].wait()
    put_weights(0)
    loads[1].wait()
    spread_x(vort, 0)
    interior_x(vort, 0)
    for t in range(2):
        svy[t] = vel[:, :, (Y - 2) * t:(Y - 2) * t + 2, :]
    svz[...] = pack([(c * X + x, vel[c, x]) for c in range(3) for x in range(X)])
    put_weights(1)
    put_weights(2)
    scale = TIME_STEP / 12.0
    for c in range(3):
        v = vel[c]
        slope[1, c] = scale * (
            8.0 * (roll(v, -1, 1) - roll(v, 1, 1)) - (roll(v, -2, 1) - roll(v, 2, 1)))
    for c in range(3):
        for x in range(2, X - 2):
            slope[0, c, x] = scale * (
                8.0 * (vel[c, x + 1] - vel[c, x - 1]) - (vel[c, x + 2] - vel[c, x - 2]))
    pl.semaphore_wait(barrier, greeted)

    diagonal, corner, face = send_x(0)
    rows = send_rows(sy.at[0], ry.at[0])
    packs = send_packs(szi.at[0], rzi.at[0])
    vrows = send_rows(svy, rvy)
    vpacks = send_packs(svz, rvz)
    vface = [
        push(vel.at[:, pl.ds((X - 2) * s, 2)], rvx.at[s], (2 * s - 1, 0, 0)) for s in range(2)
    ]
    low_lanes = lane % 4 < 2

    def merge(received, dy):
        count = 8 if dy else Y
        return jnp.where(low_lanes[:count], received[1, dy + 1, :count], received[0, dy + 1, :count])

    def stack(received):
        return jnp.concatenate([merge(received, dy) for dy in (1, 0, -1)], axis=0)

    def repeat(packed, k):
        n = 4 * X
        at = lax.broadcasted_iota(jnp.int32, packed.shape, 1)
        full = jnp.zeros(packed.shape, f32)
        for c in range(3):
            full = jnp.where((at >= c * n) & (at < (c + 1) * n), roll(packed, (c - k) * n, 1), full)
        return full

    def slopes_y():
        done(vrows)
        for c in range(3):
            top = vel[c, :, 0:4, :]
            low = rvy[1, c]
            slope[1, c, :, 0:1, :] = scale * (
                8.0 * (top[:, 1:2] - low[:, 1:2]) - (top[:, 2:3] - low[:, 0:1]))
            slope[1, c, :, 1:2, :] = scale * (
                8.0 * (top[:, 2:3] - top[:, 0:1]) - (top[:, 3:4] - low[:, 1:2]))
            end = vel[c, :, Y - 4:Y, :]
            high = rvy[0, c]
            slope[1, c, :, Y - 2:Y - 1, :] = scale * (
                8.0 * (end[:, 3:4] - end[:, 1:2]) - (high[:, 0:1] - end[:, 0:1]))
            slope[1, c, :, Y - 1:Y, :] = scale * (
                8.0 * (high[:, 0:1] - end[:, 2:3]) - (high[:, 1:2] - end[:, 1:2]))
        for s in range(2):
            w = weights(rvy[s, 1])
            wyh[s, 0] = w[3] if s else w[1]
            wyh[s, 1] = w[4] if s else w[0]

    def slopes_z(halo):
        for c in range(3):
            for x in range(X):
                v = vel[c, x]
                h = roll(halo, -(4 * (c * X + x) + 2), 1)

                def at(shift):
                    mask = lane < shift if shift > 0 else lane >= Z + shift
                    return roll(jnp.where(mask, h, v), -shift, 1)

                slope[2, c, x] = scale * (8.0 * (at(1) - at(-1)) - (at(2) - at(-2)))

    def slopes_x():
        done(vface)
        for c in range(3):
            def layer(x):
                if x < 0:
                    return rvx[1, c, x + 2]
                if x >= X:
                    return rvx[0, c, x - X]
                return vel[c, x]
            for x in (0, 1, X - 2, X - 1):
                slope[0, c, x] = scale * (
                    8.0 * (layer(x + 1) - layer(x - 1)) - (layer(x + 2) - layer(x - 2)))

    wy_packed = wz_packed = None
    for step in range(SUBSTEPS):
        if step > 0:
            spread_x(cur, step)
            diagonal, corner, face = send_x(step)
            interior_x(cur, step)
            rows = send_rows(sy.at[step], ry.at[step])
            packs = send_packs(szi.at[step], rzi.at[step])
        if step == 0:
            slopes_y()
        done(rows)
        done(corner)
        for s in range(2):
            ry[step, s, :, 0:2] += rxy[step, 1, s]
            ry[step, s, :, X - 2:X] += rxy[step, 0, s]
        done(face)
        for c in range(3):
            for x in range(2):
                cur[c, x] += rx[step, 1, c, x]
                cur[c, X - 2 + x] += rx[step, 0, c, x]

        for c in range(3):
            v = cur[c]
            keep = wgt[1, 2] * v
            for a in (-2, -1, 1, 2):
                keep = keep + roll(wgt[1, a + 2] * v, a, 1)
            cur[c] = keep
            low, high = ry[step, 1, c], ry[step, 0, c]
            near, far = wyh[1, 0] * low, wyh[1, 1] * low
            cur[c, :, 0:1, :] += near[:, 1:2] + far[:, 0:1]
            cur[c, :, 1:2, :] += far[:, 1:2]
            near, far = wyh[0, 0] * high, wyh[0, 1] * high
            cur[c, :, Y - 1:Y, :] += near[:, 0:1] + far[:, 1:2]
            cur[c, :, Y - 2:Y - 1, :] += far[:, 0:1]
        for c in range(3):
            v = cur[c]
            keep = wgt[2, 2] * v
            for a in (-2, -1, 1, 2):
                keep = keep + roll(wgt[2, a + 2] * v, a, 2)
            cur[c] = keep

        if step == 0:
            done(vpacks)
            vpacked = stack(rvz)
            wy_packed = weights(repeat(vpacked, 1))
            wz_packed = [w[8:8 + Y] for w in weights(repeat(vpacked, 2))]
            slopes_z(vpacked[8:8 + Y])
            slopes_x()

        done(packs)
        done(diagonal)
        halo = stack(rzi.at[step])
        if len(xdirs) == 1:
            halo = halo + stack(rzx.at[step, 0])
        else:
            x_of = (lax.broadcasted_iota(jnp.int32, halo.shape, 1) // 4) % X
            halo = halo + jnp.where(x_of >= X - 2, stack(rzx.at[step, 0]), 0.0)
            halo = halo + jnp.where(x_of < 2, stack(rzx.at[step, 1]), 0.0)
        spread = wy_packed[2] * halo
        for a in (-2, -1, 1, 2):
            spread = spread + roll(wy_packed[a + 2] * halo, a, 0)
        spread = spread[8:8 + Y]
        up = roll(wz_packed[4] * spread, 2, 1) + jnp.where(
            lane % 4 == 2, roll(wz_packed[3] * spread, 1, 1), 0.0)
        down = roll(wz_packed[0] * spread, -2, 1) + jnp.where(
            lane % 4 == 1, roll(wz_packed[1] * spread, -1, 1), 0.0)
        ghosts = jnp.where(low_lanes, down, up)

        final = out if step == SUBSTEPS - 1 else cur
        for x in range(X):
            v = [cur[c, x] + unpack(ghosts, c * X + x) for c in range(3)]
            for i in range(3):
                total = v[i]
                for j in range(3):
                    total = total + v[j] * slope[j, i, x]
                final[i, x] = total


def solution(mesh):
    sizes = [mesh.shape[a] for a in AXES]

    def local(vort, vel):
        _, X, Y, Z = vort.shape
        assert 12 * X <= Z and Y % 8 == 0
        f32 = jnp.float32
        V = pltpu.VMEM
        S = SUBSTEPS
        xdirs = 1 if sizes[0] == 2 else 2
        messages = S * (2 + 2 + 4 + 6 + 6 * xdirs) + 2 + 2 + 6
        return pl.pallas_call(
            functools.partial(body, sizes),
            out_shape=jax.ShapeDtypeStruct(vort.shape, f32),
            in_specs=[pl.BlockSpec(memory_space=pltpu.MemorySpace.HBM)] * 2,
            out_specs=pl.BlockSpec(memory_space=pltpu.VMEM),
            scratch_shapes=[
                V((3, X, Y, Z), f32),
                V((3, X, Y, Z), f32),
                V((3, 5, X, Y, Z), f32),
                V((3, 3, X, Y, Z), f32),
                V((3, X, Y, Z), f32),
                V((S, 2, 3, 2, Y, Z), f32),
                V((S, 2, 3, 2, Y, Z), f32),
                V((S, 2, 3, X, 2, Z), f32),
                V((S, 2, 3, X, 2, Z), f32),
                V((S, 2, 2, 3, 2, 2, Z), f32),
                V((S, 2, 2, 3, 2, 2, Z), f32),
                V((S, Y, Z), f32),
                V((S, 2, 3, Y, Z), f32),
                V((S, Y, Z), f32),
                V((S, xdirs, 2, 3, Y, Z), f32),
                V((2, 3, 2, Y, Z), f32),
                V((2, 3, X, 2, Z), f32),
                V((2, 3, X, 2, Z), f32),
                V((Y, Z), f32),
                V((2, 3, Y, Z), f32),
                V((2, 2, X, 2, Z), f32),
                pltpu.SemaphoreType.DMA((messages,)),
                pltpu.SemaphoreType.DMA((messages,)),
                pltpu.SemaphoreType.DMA((2,)),
            ],
            compiler_params=pltpu.CompilerParams(collective_id=0, has_side_effects=True),
        )(vort, vel)

    placed = P(None, *AXES)
    return jax.shard_map(
        local, mesh=mesh, in_specs=(placed, placed), out_specs=placed, check_vma=False
    )
```

```python
import functools

import jax
import jax.numpy as jnp
from jax import lax
from jax.experimental import pallas as pl
from jax.experimental.pallas import tpu as pltpu
from jax.sharding import PartitionSpec as P

SUBSTEPS = 2
TIME_STEP = 0.5
AXES = ("gx", "gy", "gz")
MESH = pl.DeviceIdType.MESH


def roll(values, shift, axis):
    return pltpu.roll(values, shift % values.shape[axis], axis)


def weights(velocity):
    d = TIME_STEP * velocity
    s = jnp.abs(d)
    t = 1.0 - s
    positive = d > 0.0
    centre = 1.0 + s * s * (1.5 * s - 2.5)
    toward = 1.0 + t * t * (1.5 * t - 2.5)
    away = -0.5 * s * t * t
    beyond = -0.5 * s * s * t
    return (
        jnp.where(positive, 0.0, beyond),
        jnp.where(positive, away, toward),
        centre,
        jnp.where(positive, toward, away),
        jnp.where(positive, beyond, 0.0),
    )


def body(
    sizes, vort_in, vel_in, out, vort, vel, wgt, slope, cur, sx, rx, sy, ry, sxy, rxy, szi, rzi, szx, rzx,
    rvx, svy, rvy, svz, rvz, wyh, send_sem, recv_sem, load_sem,
):
    _, X, Y, Z = vort.shape
    here = [lax.axis_index(a) for a in AXES]
    f32 = jnp.float32
    both = (-1, 1)
    three = (-1, 0, 1)
    xdirs = (1,) if sizes[0] == 2 else both
    used = [0]

    def device(offset):
        return tuple(
            h if o == 0 else lax.rem(h + (o if o > 0 else n + o), n)
            for h, o, n in zip(here, offset, sizes)
        )

    def push(src, dst, offset):
        index = used[0]
        used[0] += 1
        copy = pltpu.make_async_remote_copy(
            src_ref=src, dst_ref=dst, send_sem=send_sem.at[index], recv_sem=recv_sem.at[index],
            device_id=device(offset), device_id_type=MESH,
        )
        copy.start()
        return copy

    def done(copies):
        for copy in copies:
            copy.wait()

    barrier = pltpu.get_barrier_semaphore()
    greeted = 0
    for dz in three:
        for dy in three:
            for dx in (0,) + xdirs:
                if dx or dy or dz:
                    pl.semaphore_signal(
                        barrier, inc=1, device_id=device((dx, dy, dz)), device_id_type=MESH)
                    greeted += 1
    loads = [
        pltpu.make_async_copy(src, dst, load_sem.at[i])
        for i, (src, dst) in enumerate(((vel_in, vel), (vort_in, vort)))
    ]
    for load in loads:
        load.start()

    lane = lax.broadcasted_iota(jnp.int32, (Y, Z), 1)
    lane3 = lax.broadcasted_iota(jnp.int32, (X, Y, Z), 2)
    row3 = lax.broadcasted_iota(jnp.int32, (X, Y, Z), 1)
    edge = (lane < 2) | (lane >= Z - 2)

    def pack(entries):
        held = jnp.zeros((Y, Z), f32)
        for k, values in entries:
            held = jnp.where(lane // 4 == k, roll(values, 4 * k + 2, 1), held)
        return held

    def unpack(packed, k):
        return jnp.where(edge, roll(packed, -(4 * k + 2), 1), 0.0)

    def put_weights(k):
        for a, w in zip(range(-2, 3), weights(vel[k])):
            if k and a:
                at, n = (row3, Y) if k == 1 else (lane3, Z)
                w = jnp.where(at >= n - a if a > 0 else at < -a, 0.0, w)
            wgt[k, a + 2] = w

    def side_of(d):
        return (d + 1) // 2

    def tile(dy):
        return pl.ds(0, Y) if dy == 0 else pl.ds(0 if dy < 0 else Y - 8, 8)

    def spread_x(src, step):
        for c in range(3):
            sx[step, 0, c, 0] = wgt[0, 0, 0] * src[c, 0]
            sx[step, 0, c, 1] = wgt[0, 1, 0] * src[c, 0] + wgt[0, 0, 1] * src[c, 1]
            sx[step, 1, c, 0] = wgt[0, 3, X - 1] * src[c, X - 1] + wgt[0, 4, X - 2] * src[c, X - 2]
            sx[step, 1, c, 1] = wgt[0, 4, X - 1] * src[c, X - 1]
        for s in range(2):
            for t in range(2):
                sxy[step, s, t] = sx[step, s, :, :, (Y - 2) * t:(Y - 2) * t + 2, :]
        szx[step] = pack([
            (c * X + (0 if s else X - 2) + x, sx[step, s, c, x])
            for s in range(2) for c in range(3) for x in range(2)
        ])

    def interior_x(src, step):
        for c in range(3):
            layers = []
            for x in range(X):
                total = None
                for a in range(-2, 3):
                    if 0 <= x - a < X:
                        term = wgt[0, a + 2, x - a] * src[c, x - a]
                        total = term if total is None else total + term
                layers.append(total)
            for x in range(X):
                cur[c, x] = layers[x]
        for t in range(2):
            sy[step, t] = cur[:, :, (Y - 2) * t:(Y - 2) * t + 2, :]
        szi[step] = pack([(c * X + x, cur[c, x]) for c in range(3) for x in range(X)])

    def send_x(step):
        diagonal = [
            push(szx.at[step, tile(dy)],
                 rzx.at[step, i, side_of(dz), dy + 1, pl.ds(0, 8 if dy else Y)], (dx, dy, dz))
            for dy in (-1, 1, 0) for dz in both for i, dx in enumerate(xdirs)
        ]
        corner = [
            push(sxy.at[step, side_of(dx), side_of(dy)],
                 rxy.at[step, side_of(dx), side_of(dy)], (dx, dy, 0))
            for dx in both for dy in both
        ]
        face = [
            push(sx.at[step, side_of(dx)], rx.at[step, side_of(dx)], (dx, 0, 0)) for dx in both
        ]
        return diagonal, corner, face

    def send_packs(src, dst):
        return [
            push(src.at[tile(dy)], dst.at[side_of(dz), dy + 1, pl.ds(0, 8 if dy else Y)], (0, dy, dz))
            for dy in (-1, 1, 0) for dz in both
        ]

    def send_rows(src, dst):
        return [push(src.at[side_of(dy)], dst.at[side_of(dy)], (0, dy, 0)) for dy in both]

    loads[0].wait()
    put_weights(0)
    loads[1].wait()
    spread_x(vort, 0)
    interior_x(vort, 0)
    for t in range(2):
        svy[t] = vel[:, :, (Y - 2) * t:(Y - 2) * t + 2, :]
    svz[...] = pack([(c * X + x, vel[c, x]) for c in range(3) for x in range(X)])
    put_weights(1)
    put_weights(2)
    scale = TIME_STEP / 12.0
    for c in range(3):
        v = vel[c]
        slope[1, c] = scale * (
            8.0 * (roll(v, -1, 1) - roll(v, 1, 1)) - (roll(v, -2, 1) - roll(v, 2, 1)))
    for c in range(3):
        for x in range(2, X - 2):
            slope[0, c, x] = scale * (
                8.0 * (vel[c, x + 1] - vel[c, x - 1]) - (vel[c, x + 2] - vel[c, x - 2]))
    pl.semaphore_wait(barrier, greeted)

    diagonal, corner, face = send_x(0)
    rows = send_rows(sy.at[0], ry.at[0])
    packs = send_packs(szi.at[0], rzi.at[0])
    vrows = send_rows(svy, rvy)
    vpacks = send_packs(svz, rvz)
    vface = [
        push(vel.at[:, pl.ds((X - 2) * s, 2)], rvx.at[s], (2 * s - 1, 0, 0)) for s in range(2)
    ]
    low_lanes = lane % 4 < 2

    def merge(received, dy):
        count = 8 if dy else Y
        return jnp.where(low_lanes[:count], received[1, dy + 1, :count], received[0, dy + 1, :count])

    def stack(received):
        return jnp.concatenate([merge(received, dy) for dy in (1, 0, -1)], axis=0)

    def repeat(packed, k):
        n = 4 * X
        at = lax.broadcasted_iota(jnp.int32, packed.shape, 1)
        full = jnp.zeros(packed.shape, f32)
        for c in range(3):
            full = jnp.where((at >= c * n) & (at < (c + 1) * n), roll(packed, (c - k) * n, 1), full)
        return full

    def slopes_y():
        done(vrows)
        for c in range(3):
            top = vel[c, :, 0:4, :]
            low = rvy[1, c]
            slope[1, c, :, 0:1, :] = scale * (
                8.0 * (top[:, 1:2] - low[:, 1:2]) - (top[:, 2:3] - low[:, 0:1]))
            slope[1, c, :, 1:2, :] = scale * (
                8.0 * (top[:, 2:3] - top[:, 0:1]) - (top[:, 3:4] - low[:, 1:2]))
            end = vel[c, :, Y - 4:Y, :]
            high = rvy[0, c]
            slope[1, c, :, Y - 2:Y - 1, :] = scale * (
                8.0 * (end[:, 3:4] - end[:, 1:2]) - (high[:, 0:1] - end[:, 0:1]))
            slope[1, c, :, Y - 1:Y, :] = scale * (
                8.0 * (high[:, 0:1] - end[:, 2:3]) - (high[:, 1:2] - end[:, 1:2]))
        for s in range(2):
            w = weights(rvy[s, 1])
            wyh[s, 0] = w[3] if s else w[1]
            wyh[s, 1] = w[4] if s else w[0]

    def slopes_z(halo):
        for c in range(3):
            for x in range(X):
                v = vel[c, x]
                h = roll(halo, -(4 * (c * X + x) + 2), 1)

                def at(shift):
                    mask = lane < shift if shift > 0 else lane >= Z + shift
                    return roll(jnp.where(mask, h, v), -shift, 1)

                slope[2, c, x] = scale * (8.0 * (at(1) - at(-1)) - (at(2) - at(-2)))

    def slopes_x():
        done(vface)
        for c in range(3):
            def layer(x):
                if x < 0:
                    return rvx[1, c, x + 2]
                if x >= X:
                    return rvx[0, c, x - X]
                return vel[c, x]
            for x in (0, 1, X - 2, X - 1):
                slope[0, c, x] = scale * (
                    8.0 * (layer(x + 1) - layer(x - 1)) - (layer(x + 2) - layer(x - 2)))

    def remesh_yz(step, lo, hi):
        at = slice(lo, hi)
        for c in range(3):
            v = cur[c, at]
            keep = wgt[1, 2, at] * v
            for a in (-2, -1, 1, 2):
                keep = keep + roll(wgt[1, a + 2, at] * v, a, 1)
            cur[c, at] = keep
            low, high = ry[step, 1, c, at], ry[step, 0, c, at]
            near, far = wyh[1, 0, at] * low, wyh[1, 1, at] * low
            cur[c, at, 0:1, :] += near[:, 1:2] + far[:, 0:1]
            cur[c, at, 1:2, :] += far[:, 1:2]
            near, far = wyh[0, 0, at] * high, wyh[0, 1, at] * high
            cur[c, at, Y - 1:Y, :] += near[:, 0:1] + far[:, 1:2]
            cur[c, at, Y - 2:Y - 1, :] += far[:, 0:1]
        for c in range(3):
            v = cur[c, at]
            keep = wgt[2, 2, at] * v
            for a in (-2, -1, 1, 2):
                keep = keep + roll(wgt[2, a + 2, at] * v, a, 2)
            cur[c, at] = keep

    borders = (0, 1, X - 2, X - 1)
    wy_packed = wz_packed = None
    for step in range(SUBSTEPS):
        if step == 0:
            slopes_y()
        done(rows)
        remesh_yz(step, 2, X - 2)
        if step == 0:
            done(vpacks)
            vpacked = stack(rvz)
            wy_packed = weights(repeat(vpacked, 1))
            wz_packed = [w[8:8 + Y] for w in weights(repeat(vpacked, 2))]
            slopes_z(vpacked[8:8 + Y])
        done(corner)
        for s in range(2):
            ry[step, s, :, 0:2] += rxy[step, 1, s]
            ry[step, s, :, X - 2:X] += rxy[step, 0, s]
        done(face)
        for c in range(3):
            for x in range(2):
                cur[c, x] += rx[step, 1, c, x]
                cur[c, X - 2 + x] += rx[step, 0, c, x]
        remesh_yz(step, 0, 2)
        remesh_yz(step, X - 2, X)

        done(packs)
        done(diagonal)
        halo = stack(rzi.at[step])
        if len(xdirs) == 1:
            halo = halo + stack(rzx.at[step, 0])
        else:
            x_of = (lax.broadcasted_iota(jnp.int32, halo.shape, 1) // 4) % X
            halo = halo + jnp.where(x_of >= X - 2, stack(rzx.at[step, 0]), 0.0)
            halo = halo + jnp.where(x_of < 2, stack(rzx.at[step, 1]), 0.0)
        spread = wy_packed[2] * halo
        for a in (-2, -1, 1, 2):
            spread = spread + roll(wy_packed[a + 2] * halo, a, 0)
        spread = spread[8:8 + Y]
        up = roll(wz_packed[4] * spread, 2, 1) + jnp.where(
            lane % 4 == 2, roll(wz_packed[3] * spread, 1, 1), 0.0)
        down = roll(wz_packed[0] * spread, -2, 1) + jnp.where(
            lane % 4 == 1, roll(wz_packed[1] * spread, -1, 1), 0.0)
        ghosts = jnp.where(low_lanes, down, up)
        if step == 0:
            slopes_x()

        final = out if step == SUBSTEPS - 1 else cur

        def finish(x):
            v = [cur[c, x] + unpack(ghosts, c * X + x) for c in range(3)]
            for i in range(3):
                total = v[i]
                for j in range(3):
                    total = total + v[j] * slope[j, i, x]
                final[i, x] = total

        for x in borders:
            finish(x)
        if step < SUBSTEPS - 1:
            spread_x(cur, step + 1)
            diagonal, corner, face = send_x(step + 1)
        for x in range(2, X - 2):
            finish(x)
        if step < SUBSTEPS - 1:
            interior_x(cur, step + 1)
            rows = send_rows(sy.at[step + 1], ry.at[step + 1])
            packs = send_packs(szi.at[step + 1], rzi.at[step + 1])


def solution(mesh):
    sizes = [mesh.shape[a] for a in AXES]

    def local(vort, vel):
        _, X, Y, Z = vort.shape
        assert 12 * X <= Z and Y % 8 == 0
        f32 = jnp.float32
        V = pltpu.VMEM
        S = SUBSTEPS
        xdirs = 1 if sizes[0] == 2 else 2
        messages = S * (2 + 2 + 4 + 6 + 6 * xdirs) + 2 + 2 + 6
        return pl.pallas_call(
            functools.partial(body, sizes),
            out_shape=pltpu.MemorySpace.VMEM(vort.shape, f32),
            in_specs=[pl.BlockSpec(memory_space=pltpu.MemorySpace.HBM)] * 2,
            out_specs=pl.BlockSpec(memory_space=pltpu.VMEM),
            scratch_shapes=[
                V((3, X, Y, Z), f32),
                V((3, X, Y, Z), f32),
                V((3, 5, X, Y, Z), f32),
                V((3, 3, X, Y, Z), f32),
                V((3, X, Y, Z), f32),
                V((S, 2, 3, 2, Y, Z), f32),
                V((S, 2, 3, 2, Y, Z), f32),
                V((S, 2, 3, X, 2, Z), f32),
                V((S, 2, 3, X, 2, Z), f32),
                V((S, 2, 2, 3, 2, 2, Z), f32),
                V((S, 2, 2, 3, 2, 2, Z), f32),
                V((S, Y, Z), f32),
                V((S, 2, 3, Y, Z), f32),
                V((S, Y, Z), f32),
                V((S, xdirs, 2, 3, Y, Z), f32),
                V((2, 3, 2, Y, Z), f32),
                V((2, 3, X, 2, Z), f32),
                V((2, 3, X, 2, Z), f32),
                V((Y, Z), f32),
                V((2, 3, Y, Z), f32),
                V((2, 2, X, 2, Z), f32),
                pltpu.SemaphoreType.DMA((messages,)),
                pltpu.SemaphoreType.DMA((messages,)),
                pltpu.SemaphoreType.DMA((2,)),
            ],
            compiler_params=pltpu.CompilerParams(collective_id=0, has_side_effects=True),
        )(vort, vel)

    placed = P(None, *AXES)
    return jax.shard_map(
        local, mesh=mesh, in_specs=(placed, placed), out_specs=placed, check_vma=False
    )
```

```python
import functools

import jax
import jax.numpy as jnp
from jax import lax
from jax.experimental import pallas as pl
from jax.experimental.pallas import tpu as pltpu
from jax.sharding import PartitionSpec as P

SUBSTEPS = 2
TIME_STEP = 0.5
AXES = ("gx", "gy", "gz")
MESH = pl.DeviceIdType.MESH


def roll(values, shift, axis):
    return pltpu.roll(values, shift % values.shape[axis], axis)


def weights(velocity):
    d = TIME_STEP * velocity
    s = jnp.abs(d)
    t = 1.0 - s
    positive = d > 0.0
    centre = 1.0 + s * s * (1.5 * s - 2.5)
    toward = 1.0 + t * t * (1.5 * t - 2.5)
    away = -0.5 * s * t * t
    beyond = -0.5 * s * s * t
    return (
        jnp.where(positive, 0.0, beyond),
        jnp.where(positive, away, toward),
        centre,
        jnp.where(positive, toward, away),
        jnp.where(positive, beyond, 0.0),
    )


def body(
    sizes, vort_in, vel_in, out, vort, vel, wgt, slope, cur, sx, rx, sy, ry, sxy, rxy, szi, rzi, szx, rzx,
    rvx, svy, rvy, svz, rvz, wyh, send_sem, recv_sem, load_sem,
):
    _, X, Y, Z = vort.shape
    here = [lax.axis_index(a) for a in AXES]
    f32 = jnp.float32
    both = (-1, 1)
    three = (-1, 0, 1)
    xdirs = (1,) if sizes[0] == 2 else both
    used = [0]

    def device(offset):
        return tuple(
            h if o == 0 else lax.rem(h + (o if o > 0 else n + o), n)
            for h, o, n in zip(here, offset, sizes)
        )

    def push(src, dst, offset):
        index = used[0]
        used[0] += 1
        copy = pltpu.make_async_remote_copy(
            src_ref=src, dst_ref=dst, send_sem=send_sem.at[index], recv_sem=recv_sem.at[index],
            device_id=device(offset), device_id_type=MESH,
        )
        copy.start()
        return copy

    def done(copies):
        for copy in copies:
            copy.wait()

    barrier = pltpu.get_barrier_semaphore()
    greeted = 0
    for dz in three:
        for dy in three:
            for dx in (0,) + xdirs:
                if dx or dy or dz:
                    pl.semaphore_signal(
                        barrier, inc=1, device_id=device((dx, dy, dz)), device_id_type=MESH)
                    greeted += 1
    loads = [
        pltpu.make_async_copy(src, dst, load_sem.at[i])
        for i, (src, dst) in enumerate(((vel_in, vel), (vort_in, vort)))
    ]
    for load in loads:
        load.start()

    lane = lax.broadcasted_iota(jnp.int32, (Y, Z), 1)
    lane3 = lax.broadcasted_iota(jnp.int32, (X, Y, Z), 2)
    row3 = lax.broadcasted_iota(jnp.int32, (X, Y, Z), 1)
    edge = (lane < 2) | (lane >= Z - 2)

    def pack(entries):
        held = jnp.zeros((Y, Z), f32)
        for k, values in entries:
            held = jnp.where(lane // 4 == k, roll(values, 4 * k + 2, 1), held)
        return held

    def unpack(packed, k):
        return jnp.where(edge, roll(packed, -(4 * k + 2), 1), 0.0)

    def put_weights(k):
        for a, w in zip(range(-2, 3), weights(vel[k])):
            if k and a:
                at, n = (row3, Y) if k == 1 else (lane3, Z)
                w = jnp.where(at >= n - a if a > 0 else at < -a, 0.0, w)
            wgt[k, a + 2] = w

    def side_of(d):
        return (d + 1) // 2

    def tile(dy):
        return pl.ds(0, Y) if dy == 0 else pl.ds(0 if dy < 0 else Y - 2, 2)

    def slot(dy):
        return pl.ds(0, Y) if dy == 0 else pl.ds(0 if dy < 0 else 6, 2)

    def spread_x(src, step):
        for c in range(3):
            sx[step, 0, c, 0] = wgt[0, 0, 0] * src[c, 0]
            sx[step, 0, c, 1] = wgt[0, 1, 0] * src[c, 0] + wgt[0, 0, 1] * src[c, 1]
            sx[step, 1, c, 0] = wgt[0, 3, X - 1] * src[c, X - 1] + wgt[0, 4, X - 2] * src[c, X - 2]
            sx[step, 1, c, 1] = wgt[0, 4, X - 1] * src[c, X - 1]
        for s in range(2):
            for t in range(2):
                sxy[step, s, t] = sx[step, s, :, :, (Y - 2) * t:(Y - 2) * t + 2, :]
        szx[step] = pack([
            (c * X + (0 if s else X - 2) + x, sx[step, s, c, x])
            for s in range(2) for c in range(3) for x in range(2)
        ])

    def interior_x(src, step):
        for c in range(3):
            layers = []
            for x in range(X):
                total = None
                for a in range(-2, 3):
                    if 0 <= x - a < X:
                        term = wgt[0, a + 2, x - a] * src[c, x - a]
                        total = term if total is None else total + term
                layers.append(total)
            for x in range(X):
                cur[c, x] = layers[x]
        for t in range(2):
            sy[step, t] = cur[:, :, (Y - 2) * t:(Y - 2) * t + 2, :]
        szi[step] = pack([(c * X + x, cur[c, x]) for c in range(3) for x in range(X)])

    def send_x(step):
        diagonal = [
            push(szx.at[step, tile(dy)],
                 rzx.at[step, i, side_of(dz), dy + 1, slot(dy)], (dx, dy, dz))
            for dy in (-1, 1, 0) for dz in both for i, dx in enumerate(xdirs)
        ]
        face = [
            push(sx.at[step, side_of(dx)], rx.at[step, side_of(dx)], (dx, 0, 0)) for dx in both
        ]
        corner = [
            push(sxy.at[step, side_of(dx), side_of(dy)],
                 rxy.at[step, side_of(dx), side_of(dy)], (dx, dy, 0))
            for dx in both for dy in both
        ]
        return diagonal, corner, face

    def send_packs(src, dst):
        return [
            push(src.at[tile(dy)], dst.at[side_of(dz), dy + 1, slot(dy)], (0, dy, dz))
            for dy in (-1, 1, 0) for dz in both
        ]

    def send_rows(src, dst):
        return [push(src.at[side_of(dy)], dst.at[side_of(dy)], (0, dy, 0)) for dy in both]

    loads[0].wait()
    put_weights(0)
    loads[1].wait()
    spread_x(vort, 0)
    interior_x(vort, 0)
    for t in range(2):
        svy[t] = vel[:, :, (Y - 2) * t:(Y - 2) * t + 2, :]
    svz[...] = pack([(c * X + x, vel[c, x]) for c in range(3) for x in range(X)])
    put_weights(1)
    put_weights(2)
    scale = TIME_STEP / 12.0
    for c in range(3):
        v = vel[c]
        slope[1, c] = scale * (
            8.0 * (roll(v, -1, 1) - roll(v, 1, 1)) - (roll(v, -2, 1) - roll(v, 2, 1)))
    for c in range(3):
        for x in range(2, X - 2):
            slope[0, c, x] = scale * (
                8.0 * (vel[c, x + 1] - vel[c, x - 1]) - (vel[c, x + 2] - vel[c, x - 2]))
    pl.semaphore_wait(barrier, greeted)

    diagonal, corner, face = send_x(0)
    rows = send_rows(sy.at[0], ry.at[0])
    packs = send_packs(szi.at[0], rzi.at[0])
    vrows = send_rows(svy, rvy)
    vpacks = send_packs(svz, rvz)
    vface = [
        push(vel.at[:, pl.ds((X - 2) * s, 2)], rvx.at[s], (2 * s - 1, 0, 0)) for s in range(2)
    ]
    low_lanes = lane % 4 < 2

    def merge(received, dy):
        count = 8 if dy else Y
        return jnp.where(low_lanes[:count], received[1, dy + 1, :count], received[0, dy + 1, :count])

    def stack(received):
        return jnp.concatenate([merge(received, dy) for dy in (1, 0, -1)], axis=0)

    def repeat(packed, k):
        n = 4 * X
        at = lax.broadcasted_iota(jnp.int32, packed.shape, 1)
        full = jnp.zeros(packed.shape, f32)
        for c in range(3):
            full = jnp.where((at >= c * n) & (at < (c + 1) * n), roll(packed, (c - k) * n, 1), full)
        return full

    def slopes_y():
        done(vrows)
        for c in range(3):
            top = vel[c, :, 0:4, :]
            low = rvy[1, c]
            slope[1, c, :, 0:1, :] = scale * (
                8.0 * (top[:, 1:2] - low[:, 1:2]) - (top[:, 2:3] - low[:, 0:1]))
            slope[1, c, :, 1:2, :] = scale * (
                8.0 * (top[:, 2:3] - top[:, 0:1]) - (top[:, 3:4] - low[:, 1:2]))
            end = vel[c, :, Y - 4:Y, :]
            high = rvy[0, c]
            slope[1, c, :, Y - 2:Y - 1, :] = scale * (
                8.0 * (end[:, 3:4] - end[:, 1:2]) - (high[:, 0:1] - end[:, 0:1]))
            slope[1, c, :, Y - 1:Y, :] = scale * (
                8.0 * (high[:, 0:1] - end[:, 2:3]) - (high[:, 1:2] - end[:, 1:2]))
        for s in range(2):
            w = weights(rvy[s, 1])
            wyh[s, 0] = w[3] if s else w[1]
            wyh[s, 1] = w[4] if s else w[0]

    def slopes_z(halo):
        for c in range(3):
            for x in range(X):
                v = vel[c, x]
                h = roll(halo, -(4 * (c * X + x) + 2), 1)

                def at(shift):
                    mask = lane < shift if shift > 0 else lane >= Z + shift
                    return roll(jnp.where(mask, h, v), -shift, 1)

                slope[2, c, x] = scale * (8.0 * (at(1) - at(-1)) - (at(2) - at(-2)))

    def slopes_x():
        done(vface)
        for c in range(3):
            def layer(x):
                if x < 0:
                    return rvx[1, c, x + 2]
                if x >= X:
                    return rvx[0, c, x - X]
                return vel[c, x]
            for x in (0, 1, X - 2, X - 1):
                slope[0, c, x] = scale * (
                    8.0 * (layer(x + 1) - layer(x - 1)) - (layer(x + 2) - layer(x - 2)))

    def remesh_yz(step, lo, hi):
        at = slice(lo, hi)
        for c in range(3):
            v = cur[c, at]
            keep = wgt[1, 2, at] * v
            for a in (-2, -1, 1, 2):
                keep = keep + roll(wgt[1, a + 2, at] * v, a, 1)
            cur[c, at] = keep
            low, high = ry[step, 1, c, at], ry[step, 0, c, at]
            near, far = wyh[1, 0, at] * low, wyh[1, 1, at] * low
            cur[c, at, 0:1, :] += near[:, 1:2] + far[:, 0:1]
            cur[c, at, 1:2, :] += far[:, 1:2]
            near, far = wyh[0, 0, at] * high, wyh[0, 1, at] * high
            cur[c, at, Y - 1:Y, :] += near[:, 0:1] + far[:, 1:2]
            cur[c, at, Y - 2:Y - 1, :] += far[:, 0:1]
        for c in range(3):
            v = cur[c, at]
            keep = wgt[2, 2, at] * v
            for a in (-2, -1, 1, 2):
                keep = keep + roll(wgt[2, a + 2, at] * v, a, 2)
            cur[c, at] = keep

    borders = (0, 1, X - 2, X - 1)
    wy_packed = wz_packed = None
    for step in range(SUBSTEPS):
        if step == 0:
            slopes_y()
        done(rows)
        remesh_yz(step, 2, X - 2)
        if step == 0:
            done(vpacks)
            vpacked = stack(rvz)
            wy_packed = weights(repeat(vpacked, 1))
            wz_packed = [w[8:8 + Y] for w in weights(repeat(vpacked, 2))]
            slopes_z(vpacked[8:8 + Y])
        done(corner)
        for s in range(2):
            ry[step, s, :, 0:2] += rxy[step, 1, s]
            ry[step, s, :, X - 2:X] += rxy[step, 0, s]
        done(face)
        for c in range(3):
            for x in range(2):
                cur[c, x] += rx[step, 1, c, x]
                cur[c, X - 2 + x] += rx[step, 0, c, x]
        remesh_yz(step, 0, 2)
        remesh_yz(step, X - 2, X)

        done(packs)
        done(diagonal)
        halo = stack(rzi.at[step])
        if len(xdirs) == 1:
            halo = halo + stack(rzx.at[step, 0])
        else:
            x_of = (lax.broadcasted_iota(jnp.int32, halo.shape, 1) // 4) % X
            halo = halo + jnp.where(x_of >= X - 2, stack(rzx.at[step, 0]), 0.0)
            halo = halo + jnp.where(x_of < 2, stack(rzx.at[step, 1]), 0.0)
        spread = wy_packed[2] * halo
        for a in (-2, -1, 1, 2):
            spread = spread + roll(wy_packed[a + 2] * halo, a, 0)
        spread = spread[8:8 + Y]
        up = roll(wz_packed[4] * spread, 2, 1) + jnp.where(
            lane % 4 == 2, roll(wz_packed[3] * spread, 1, 1), 0.0)
        down = roll(wz_packed[0] * spread, -2, 1) + jnp.where(
            lane % 4 == 1, roll(wz_packed[1] * spread, -1, 1), 0.0)
        ghosts = jnp.where(low_lanes, down, up)
        if step == 0:
            slopes_x()

        final = out if step == SUBSTEPS - 1 else cur

        def finish(x):
            v = [cur[c, x] + unpack(ghosts, c * X + x) for c in range(3)]
            for i in range(3):
                total = v[i]
                for j in range(3):
                    total = total + v[j] * slope[j, i, x]
                final[i, x] = total

        for x in borders:
            finish(x)
        if step < SUBSTEPS - 1:
            spread_x(cur, step + 1)
            diagonal, corner, face = send_x(step + 1)
        for x in range(2, X - 2):
            finish(x)
        if step < SUBSTEPS - 1:
            interior_x(cur, step + 1)
            rows = send_rows(sy.at[step + 1], ry.at[step + 1])
            packs = send_packs(szi.at[step + 1], rzi.at[step + 1])


def solution(mesh):
    sizes = [mesh.shape[a] for a in AXES]

    def local(vort, vel):
        _, X, Y, Z = vort.shape
        assert 12 * X <= Z and Y % 8 == 0
        f32 = jnp.float32
        V = pltpu.VMEM
        S = SUBSTEPS
        xdirs = 1 if sizes[0] == 2 else 2
        messages = S * (2 + 2 + 4 + 6 + 6 * xdirs) + 2 + 2 + 6
        return pl.pallas_call(
            functools.partial(body, sizes),
            out_shape=pltpu.MemorySpace.VMEM(vort.shape, f32),
            in_specs=[pl.BlockSpec(memory_space=pltpu.MemorySpace.HBM)] * 2,
            out_specs=pl.BlockSpec(memory_space=pltpu.VMEM),
            scratch_shapes=[
                V((3, X, Y, Z), f32),
                V((3, X, Y, Z), f32),
                V((3, 5, X, Y, Z), f32),
                V((3, 3, X, Y, Z), f32),
                V((3, X, Y, Z), f32),
                V((S, 2, 3, 2, Y, Z), f32),
                V((S, 2, 3, 2, Y, Z), f32),
                V((S, 2, 3, X, 2, Z), f32),
                V((S, 2, 3, X, 2, Z), f32),
                V((S, 2, 2, 3, 2, 2, Z), f32),
                V((S, 2, 2, 3, 2, 2, Z), f32),
                V((S, Y, Z), f32),
                V((S, 2, 3, Y, Z), f32),
                V((S, Y, Z), f32),
                V((S, xdirs, 2, 3, Y, Z), f32),
                V((2, 3, 2, Y, Z), f32),
                V((2, 3, X, 2, Z), f32),
                V((2, 3, X, 2, Z), f32),
                V((Y, Z), f32),
                V((2, 3, Y, Z), f32),
                V((2, 2, X, 2, Z), f32),
                pltpu.SemaphoreType.DMA((messages,)),
                pltpu.SemaphoreType.DMA((messages,)),
                pltpu.SemaphoreType.DMA((2,)),
            ],
            compiler_params=pltpu.CompilerParams(collective_id=0, has_side_effects=True),
        )(vort, vel)

    placed = P(None, *AXES)
    return jax.shard_map(
        local, mesh=mesh, in_specs=(placed, placed), out_specs=placed, check_vma=False
    )
```

```python
import functools

import jax
import jax.numpy as jnp
from jax import lax
from jax.experimental import pallas as pl
from jax.experimental.pallas import tpu as pltpu
from jax.sharding import PartitionSpec as P

SUBSTEPS = 2
TIME_STEP = 0.5
AXES = ("gx", "gy", "gz")
MESH = pl.DeviceIdType.MESH


def roll(values, shift, axis):
    return pltpu.roll(values, shift % values.shape[axis], axis)


def weights(velocity):
    d = TIME_STEP * velocity
    s = jnp.abs(d)
    t = 1.0 - s
    positive = d > 0.0
    centre = 1.0 + s * s * (1.5 * s - 2.5)
    toward = 1.0 + t * t * (1.5 * t - 2.5)
    away = -0.5 * s * t * t
    beyond = -0.5 * s * s * t
    return (
        jnp.where(positive, 0.0, beyond),
        jnp.where(positive, away, toward),
        centre,
        jnp.where(positive, toward, away),
        jnp.where(positive, beyond, 0.0),
    )


def body(
    sizes, vort_in, vel_in, out, vort, vel, wgt, slope, cur, sx, rx, sy, ry, sxy, rxy, szi, rzi, szx, rzx,
    rvx, svy, rvy, svz, rvz, wyh, send_sem, recv_sem, load_sem,
):
    _, X, Y, Z = vort.shape
    here = [lax.axis_index(a) for a in AXES]
    f32 = jnp.float32
    both = (-1, 1)
    three = (-1, 0, 1)
    xdirs = (1,) if sizes[0] == 2 else both
    used = [0]

    def device(offset):
        return tuple(
            h if o == 0 else lax.rem(h + (o if o > 0 else n + o), n)
            for h, o, n in zip(here, offset, sizes)
        )

    def push(src, dst, offset):
        index = used[0]
        used[0] += 1
        copy = pltpu.make_async_remote_copy(
            src_ref=src, dst_ref=dst, send_sem=send_sem.at[index], recv_sem=recv_sem.at[index],
            device_id=device(offset), device_id_type=MESH,
        )
        copy.start()
        return copy

    def done(copies):
        for copy in copies:
            copy.wait()

    barrier = pltpu.get_barrier_semaphore()
    greeted = 0
    for dz in three:
        for dy in three:
            for dx in (0,) + xdirs:
                if dx or dy or dz:
                    pl.semaphore_signal(
                        barrier, inc=1, device_id=device((dx, dy, dz)), device_id_type=MESH)
                    greeted += 1
    loads = [
        pltpu.make_async_copy(src, dst, load_sem.at[i])
        for i, (src, dst) in enumerate(((vel_in, vel), (vort_in, vort)))
    ]
    for load in loads:
        load.start()

    lane = lax.broadcasted_iota(jnp.int32, (Y, Z), 1)
    lane3 = lax.broadcasted_iota(jnp.int32, (X, Y, Z), 2)
    row3 = lax.broadcasted_iota(jnp.int32, (X, Y, Z), 1)
    edge = (lane < 2) | (lane >= Z - 2)

    def pack(entries):
        held = jnp.zeros((Y, Z), f32)
        for k, values in entries:
            held = jnp.where(lane // 4 == k, roll(values, 4 * k + 2, 1), held)
        return held

    def unpack(packed, k):
        return jnp.where(edge, roll(packed, -(4 * k + 2), 1), 0.0)

    def put_weights(k):
        for a, w in zip(range(-2, 3), weights(vel[k])):
            if k and a:
                at, n = (row3, Y) if k == 1 else (lane3, Z)
                w = jnp.where(at >= n - a if a > 0 else at < -a, 0.0, w)
            wgt[k, a + 2] = w

    def side_of(d):
        return (d + 1) // 2

    def tile(dy):
        return pl.ds(0, Y) if dy == 0 else pl.ds(0 if dy < 0 else Y - 2, 2)

    def slot(dy):
        return pl.ds(0, Y) if dy == 0 else pl.ds(0 if dy < 0 else 6, 2)

    def spread_x(src, step):
        for c in range(3):
            sx[step, 0, c, 0] = wgt[0, 0, 0] * src[c, 0]
            sx[step, 0, c, 1] = wgt[0, 1, 0] * src[c, 0] + wgt[0, 0, 1] * src[c, 1]
            sx[step, 1, c, 0] = wgt[0, 3, X - 1] * src[c, X - 1] + wgt[0, 4, X - 2] * src[c, X - 2]
            sx[step, 1, c, 1] = wgt[0, 4, X - 1] * src[c, X - 1]
        for s in range(2):
            for t in range(2):
                sxy[step, s, t] = sx[step, s, :, :, (Y - 2) * t:(Y - 2) * t + 2, :]
        szx[step] = pack([
            (c * X + (0 if s else X - 2) + x, sx[step, s, c, x])
            for s in range(2) for c in range(3) for x in range(2)
        ])

    def interior_x(src, step):
        for c in range(3):
            layers = []
            for x in range(X):
                total = None
                for a in range(-2, 3):
                    if 0 <= x - a < X:
                        term = wgt[0, a + 2, x - a] * src[c, x - a]
                        total = term if total is None else total + term
                layers.append(total)
            for x in range(X):
                cur[c, x] = layers[x]
        for t in range(2):
            sy[step, t] = cur[:, :, (Y - 2) * t:(Y - 2) * t + 2, :]
        szi[step] = pack([(c * X + x, cur[c, x]) for c in range(3) for x in range(X)])

    def send_x(step):
        diagonal = [
            push(szx.at[step, tile(dy)],
                 rzx.at[step, i, side_of(dz), dy + 1, slot(dy)], (dx, dy, dz))
            for dy in (-1, 1, 0) for dz in both for i, dx in enumerate(xdirs)
        ]
        face = [
            push(sx.at[step, side_of(dx)], rx.at[step, side_of(dx)], (dx, 0, 0)) for dx in both
        ]
        corner = [
            push(sxy.at[step, side_of(dx), side_of(dy)],
                 rxy.at[step, side_of(dx), side_of(dy)], (dx, dy, 0))
            for dx in both for dy in both
        ]
        return diagonal, corner, face

    def send_packs(src, dst):
        return [
            push(src.at[tile(dy)], dst.at[side_of(dz), dy + 1, slot(dy)], (0, dy, dz))
            for dy in (-1, 1, 0) for dz in both
        ]

    def send_rows(src, dst):
        return [push(src.at[side_of(dy)], dst.at[side_of(dy)], (0, dy, 0)) for dy in both]

    loads[0].wait()
    put_weights(0)
    loads[1].wait()
    spread_x(vort, 0)
    interior_x(vort, 0)
    for t in range(2):
        svy[t] = vel[:, :, (Y - 2) * t:(Y - 2) * t + 2, :]
    svz[...] = pack([(c * X + x, vel[c, x]) for c in range(3) for x in range(X)])
    put_weights(1)
    put_weights(2)
    scale = TIME_STEP / 12.0
    for c in range(3):
        v = vel[c]
        slope[1, c] = scale * (
            8.0 * (roll(v, -1, 1) - roll(v, 1, 1)) - (roll(v, -2, 1) - roll(v, 2, 1)))
    for c in range(3):
        for x in range(2, X - 2):
            slope[0, c, x] = scale * (
                8.0 * (vel[c, x + 1] - vel[c, x - 1]) - (vel[c, x + 2] - vel[c, x - 2]))
    pl.semaphore_wait(barrier, greeted)

    diagonal, corner, face = send_x(0)
    rows = send_rows(sy.at[0], ry.at[0])
    packs = send_packs(szi.at[0], rzi.at[0])
    vrows = send_rows(svy, rvy)
    vpacks = send_packs(svz, rvz)
    vface = [
        push(vel.at[:, pl.ds((X - 2) * s, 2)], rvx.at[s], (2 * s - 1, 0, 0)) for s in range(2)
    ]
    low_lanes = lane % 4 < 2

    def merge(received, dy):
        count = 8 if dy else Y
        return jnp.where(low_lanes[:count], received[1, dy + 1, :count], received[0, dy + 1, :count])

    def stack(received):
        return jnp.concatenate([merge(received, dy) for dy in (1, 0, -1)], axis=0)

    def repeat(packed, k):
        n = 4 * X
        at = lax.broadcasted_iota(jnp.int32, packed.shape, 1)
        full = jnp.zeros(packed.shape, f32)
        for c in range(3):
            full = jnp.where((at >= c * n) & (at < (c + 1) * n), roll(packed, (c - k) * n, 1), full)
        return full

    def slopes_y():
        done(vrows)
        for c in range(3):
            top = vel[c, :, 0:4, :]
            low = rvy[1, c]
            slope[1, c, :, 0:1, :] = scale * (
                8.0 * (top[:, 1:2] - low[:, 1:2]) - (top[:, 2:3] - low[:, 0:1]))
            slope[1, c, :, 1:2, :] = scale * (
                8.0 * (top[:, 2:3] - top[:, 0:1]) - (top[:, 3:4] - low[:, 1:2]))
            end = vel[c, :, Y - 4:Y, :]
            high = rvy[0, c]
            slope[1, c, :, Y - 2:Y - 1, :] = scale * (
                8.0 * (end[:, 3:4] - end[:, 1:2]) - (high[:, 0:1] - end[:, 0:1]))
            slope[1, c, :, Y - 1:Y, :] = scale * (
                8.0 * (high[:, 0:1] - end[:, 2:3]) - (high[:, 1:2] - end[:, 1:2]))
        for s in range(2):
            w = weights(rvy[s, 1])
            wyh[s, 0] = w[3] if s else w[1]
            wyh[s, 1] = w[4] if s else w[0]

    def slopes_z(halo):
        for c in range(3):
            for x in range(X):
                v = vel[c, x]
                h = roll(halo, -(4 * (c * X + x) + 2), 1)

                def at(shift):
                    mask = lane < shift if shift > 0 else lane >= Z + shift
                    return roll(jnp.where(mask, h, v), -shift, 1)

                slope[2, c, x] = scale * (8.0 * (at(1) - at(-1)) - (at(2) - at(-2)))

    def slopes_x():
        done(vface)
        for c in range(3):
            def layer(x):
                if x < 0:
                    return rvx[1, c, x + 2]
                if x >= X:
                    return rvx[0, c, x - X]
                return vel[c, x]
            for x in (0, 1, X - 2, X - 1):
                slope[0, c, x] = scale * (
                    8.0 * (layer(x + 1) - layer(x - 1)) - (layer(x + 2) - layer(x - 2)))

    def remesh_yz(step, lo, hi):
        at = slice(lo, hi)
        for c in range(3):
            v = cur[c, at]
            keep = wgt[1, 2, at] * v
            for a in (-2, -1, 1, 2):
                keep = keep + roll(wgt[1, a + 2, at] * v, a, 1)
            cur[c, at] = keep
            low, high = ry[step, 1, c, at], ry[step, 0, c, at]
            near, far = wyh[1, 0, at] * low, wyh[1, 1, at] * low
            cur[c, at, 0:1, :] += near[:, 1:2] + far[:, 0:1]
            cur[c, at, 1:2, :] += far[:, 1:2]
            near, far = wyh[0, 0, at] * high, wyh[0, 1, at] * high
            cur[c, at, Y - 1:Y, :] += near[:, 0:1] + far[:, 1:2]
            cur[c, at, Y - 2:Y - 1, :] += far[:, 0:1]
        for c in range(3):
            v = cur[c, at]
            keep = wgt[2, 2, at] * v
            for a in (-2, -1, 1, 2):
                keep = keep + roll(wgt[2, a + 2, at] * v, a, 2)
            cur[c, at] = keep

    borders = (0, 1, X - 2, X - 1)
    wy_packed = wz_packed = None
    for step in range(SUBSTEPS):
        if step == 0:
            slopes_y()
        done(rows)
        remesh_yz(step, 2, X - 2)
        done(corner)
        for s in range(2):
            ry[step, s, :, 0:2] += rxy[step, 1, s]
            ry[step, s, :, X - 2:X] += rxy[step, 0, s]
        done(face)
        for c in range(3):
            for x in range(2):
                cur[c, x] += rx[step, 1, c, x]
                cur[c, X - 2 + x] += rx[step, 0, c, x]
        remesh_yz(step, 0, 2)
        remesh_yz(step, X - 2, X)

        if step == 0:
            done(vpacks)
            vpacked = stack(rvz)
            wy_packed = weights(repeat(vpacked, 1))
            wz_packed = [w[8:8 + Y] for w in weights(repeat(vpacked, 2))]
            slopes_z(vpacked[8:8 + Y])

        done(packs)
        done(diagonal)
        halo = stack(rzi.at[step])
        if len(xdirs) == 1:
            halo = halo + stack(rzx.at[step, 0])
        else:
            x_of = (lax.broadcasted_iota(jnp.int32, halo.shape, 1) // 4) % X
            halo = halo + jnp.where(x_of >= X - 2, stack(rzx.at[step, 0]), 0.0)
            halo = halo + jnp.where(x_of < 2, stack(rzx.at[step, 1]), 0.0)
        spread = wy_packed[2] * halo
        for a in (-2, -1, 1, 2):
            spread = spread + roll(wy_packed[a + 2] * halo, a, 0)
        spread = spread[8:8 + Y]
        up = roll(wz_packed[4] * spread, 2, 1) + jnp.where(
            lane % 4 == 2, roll(wz_packed[3] * spread, 1, 1), 0.0)
        down = roll(wz_packed[0] * spread, -2, 1) + jnp.where(
            lane % 4 == 1, roll(wz_packed[1] * spread, -1, 1), 0.0)
        ghosts = jnp.where(low_lanes, down, up)
        if step == 0:
            slopes_x()

        final = out if step == SUBSTEPS - 1 else cur

        def finish(x):
            v = [cur[c, x] + unpack(ghosts, c * X + x) for c in range(3)]
            for i in range(3):
                total = v[i]
                for j in range(3):
                    total = total + v[j] * slope[j, i, x]
                final[i, x] = total

        for x in borders:
            finish(x)
        if step < SUBSTEPS - 1:
            spread_x(cur, step + 1)
            diagonal, corner, face = send_x(step + 1)
        for x in range(2, X - 2):
            finish(x)
        if step < SUBSTEPS - 1:
            interior_x(cur, step + 1)
            rows = send_rows(sy.at[step + 1], ry.at[step + 1])
            packs = send_packs(szi.at[step + 1], rzi.at[step + 1])


def solution(mesh):
    sizes = [mesh.shape[a] for a in AXES]

    def local(vort, vel):
        _, X, Y, Z = vort.shape
        assert 12 * X <= Z and Y % 8 == 0
        f32 = jnp.float32
        V = pltpu.VMEM
        S = SUBSTEPS
        xdirs = 1 if sizes[0] == 2 else 2
        messages = S * (2 + 2 + 4 + 6 + 6 * xdirs) + 2 + 2 + 6
        return pl.pallas_call(
            functools.partial(body, sizes),
            out_shape=pltpu.MemorySpace.VMEM(vort.shape, f32),
            in_specs=[pl.BlockSpec(memory_space=pltpu.MemorySpace.HBM)] * 2,
            out_specs=pl.BlockSpec(memory_space=pltpu.VMEM),
            scratch_shapes=[
                V((3, X, Y, Z), f32),
                V((3, X, Y, Z), f32),
                V((3, 5, X, Y, Z), f32),
                V((3, 3, X, Y, Z), f32),
                V((3, X, Y, Z), f32),
                V((S, 2, 3, 2, Y, Z), f32),
                V((S, 2, 3, 2, Y, Z), f32),
                V((S, 2, 3, X, 2, Z), f32),
                V((S, 2, 3, X, 2, Z), f32),
                V((S, 2, 2, 3, 2, 2, Z), f32),
                V((S, 2, 2, 3, 2, 2, Z), f32),
                V((S, Y, Z), f32),
                V((S, 2, 3, Y, Z), f32),
                V((S, Y, Z), f32),
                V((S, xdirs, 2, 3, Y, Z), f32),
                V((2, 3, 2, Y, Z), f32),
                V((2, 3, X, 2, Z), f32),
                V((2, 3, X, 2, Z), f32),
                V((Y, Z), f32),
                V((2, 3, Y, Z), f32),
                V((2, 2, X, 2, Z), f32),
                pltpu.SemaphoreType.DMA((messages,)),
                pltpu.SemaphoreType.DMA((messages,)),
                pltpu.SemaphoreType.DMA((2,)),
            ],
            compiler_params=pltpu.CompilerParams(collective_id=0, has_side_effects=True),
        )(vort, vel)

    placed = P(None, *AXES)
    return jax.shard_map(
        local, mesh=mesh, in_specs=(placed, placed), out_specs=placed, check_vma=False
    )
```
